16 devices in a mesh: data: 4 (over z, y), tp: 4 (over x, core).
Axes of the slice: x: 2, y: 2, z: 2, core: 2. Of those that a mesh axis runs over, the one named last changes fastest.
Arguments:
- x_all: bfloat16 [256, 2560], P(('data', 'tp')), parts along dimension 0
- ln_gammas: float32 [2, 2560], replicated
- w_in: bfloat16 [2, 2560, 10240], P(None, None, 'tp')
- w_out: bfloat16 [2, 10240, 2560], P(None, 'tp')
Outputs:
- output: bfloat16 [256, 2560], P(('data', 'tp')), parts along dimension 0
There are 4 independent parts. The reference program is written for one: setup_inputs(seed, part) draws one part's arguments, and reference() takes and returns one part's arrays. A program takes and returns all parts, laid end to end along the dimension named above; an argument that names none is the same for every part.
All inputs are finite; a program needn't handle non-finite values.
Results may differ from the reference program's by a relative error of at most 0.0100232.
Values are sent between devices in bfloat16 or wider.
A program may use at most 1 GiB of HBM per device.

```python
import math
import jax
import jax.numpy as jnp
from jax import lax

SEQ_LEN = 64
D_MODEL = 2560
FF_WIDTH = 10240
NUM_LAYERS = 2

LN_EPS = 1e-6
ROW_BLOCK = math.gcd(SEQ_LEN, 512)


def setup_inputs(seed: int = 0, part: int = 0) -> dict:
    part_key = jax.random.fold_in(jax.random.key(seed), part)
    shared_key = jax.random.key(seed + 1)
    key_gamma, key_in, key_out = jax.random.split(shared_key, 3)
    x_all = jax.random.normal(part_key, (SEQ_LEN, D_MODEL), jnp.float32).astype(jnp.bfloat16)
    ln_gammas = 1.0 + 0.25 * jax.random.normal(key_gamma, (NUM_LAYERS, D_MODEL), jnp.float32)
    w_in = (jax.random.normal(key_in, (NUM_LAYERS, D_MODEL, FF_WIDTH), jnp.float32) * D_MODEL ** -0.5).astype(jnp.bfloat16)
    w_out = (jax.random.normal(key_out, (NUM_LAYERS, FF_WIDTH, D_MODEL), jnp.float32) * (1.5 * FF_WIDTH ** -0.5)).astype(jnp.bfloat16)
    return {"x_all": x_all, "ln_gammas": ln_gammas, "w_in": w_in, "w_out": w_out}


def mlp_layer(x_rows, gamma_row, w_in_layer, w_out_layer):
    x_f32 = x_rows.astype(jnp.float32)
    mean_val = jnp.mean(x_f32, axis=-1, keepdims=True)
    centered = x_f32 - mean_val
    var_val = jnp.mean(centered * centered, axis=-1, keepdims=True)
    normed = (centered * lax.rsqrt(var_val + LN_EPS) * gamma_row).astype(jnp.bfloat16)
    hidden = jax.nn.gelu(jnp.dot(normed, w_in_layer, preferred_element_type=jnp.float32), approximate=True).astype(jnp.bfloat16)
    mlp_out = jnp.dot(hidden, w_out_layer, preferred_element_type=jnp.float32)
    return (x_f32 + mlp_out).astype(jnp.bfloat16)


def reference(x_all, ln_gammas, w_in, w_out):
    row_blocks = x_all.reshape(SEQ_LEN // ROW_BLOCK, ROW_BLOCK, D_MODEL)

    def run_block(rows):
        def layer_step(carry, layer_params):
            gamma_row, w_in_layer, w_out_layer = layer_params
            return mlp_layer(carry, gamma_row, w_in_layer, w_out_layer), None
        final_rows, _ = lax.scan(layer_step, rows, (ln_gammas, w_in, w_out))
        return final_rows

    return lax.map(run_block, row_blocks).reshape(SEQ_LEN, D_MODEL)
```

```python
import functools
import jax
import jax.numpy as jnp
from jax import lax
from jax.experimental import pallas as pl
from jax.experimental.pallas import tpu as pltpu
from jax.sharding import PartitionSpec as P

LN_EPS = 1e-6
MESH = pl.DeviceIdType.MESH

BW1 = 512
BW2 = 256
GW = 1280
LAG_SUM = (1, 3)
LAG_OUT = (4, 10)
LAG_RELAY = (7, 10)


def normalize(rows_f32, gamma_row):
    mean_val = jnp.mean(rows_f32, axis=-1, keepdims=True)
    centered = rows_f32 - mean_val
    var_val = jnp.mean(centered * centered, axis=-1, keepdims=True)
    return (centered * lax.rsqrt(var_val + LN_EPS) * gamma_row).astype(jnp.bfloat16)


def kernel(x_hbm, gam_hbm, w_in, w_out, out_ref,
           wv, x_own, gam, xg, xn, h, part, part_in, sum_out, sum_in, yg,
           lsem, wsem1, wsem2, g_sem, d2d_sem, ici_sem, y_sem):
    n_layers, width, ff = w_in.shape
    n1, n2, ng = ff // BW1, width // BW2, width // GW
    me = lax.axis_index("tp")
    chip, core = lax.div(me, 2), lax.rem(me, 2)
    mate = {"tp": chip * 2 + (1 - core)}
    peer = {"tp": (1 - chip) * 2 + core}
    R = x_own.shape[0]
    mine = core * 2 + chip
    across = core * 2 + (1 - chip)

    def rows(block, n=1):
        return pl.ds(pl.multiple_of(block * R, R), n * R)

    load_x = pltpu.make_async_copy(x_hbm, x_own, lsem.at[0])
    load_g = pltpu.make_async_copy(gam_hbm, gam, lsem.at[1])
    load_x.start()
    load_g.start()
    loads1, loads2 = {}, {}
    for l in range(n_layers):
        for j in range(n1):
            cols = pl.ds(j * BW1, BW1)
            loads1[l, j] = pltpu.make_async_copy(
                w_in.at[l, :, cols], wv.at[2 * l, :, cols], wsem1.at[l, j])
            loads1[l, j].start()
        for j in range(n2):
            cols = pl.ds(j * BW2, BW2)
            loads2[l, j] = pltpu.make_async_copy(
                w_out.at[l, :, cols], wv.at[2 * l + 1, :, cols], wsem2.at[l, j])
            loads2[l, j].start()

    barrier = pltpu.get_barrier_semaphore()
    for other in (mate, peer):
        pl.semaphore_signal(barrier, inc=1, device_id=other, device_id_type=MESH)

    sends = []

    def remote(src, dst, sems, device, *idx):
        copy = pltpu.make_async_remote_copy(
            src_ref=src, dst_ref=dst, send_sem=sems.at[(0,) + idx], recv_sem=sems.at[(1,) + idx],
            device_id=device, device_id_type=MESH)
        return copy

    def launch(copy):
        copy.start()
        sends.append(copy)

    load_x.wait()
    load_g.wait()
    own = normalize(x_own[...].astype(jnp.float32), gam[0:1, :])
    for g in range(ng):
        xg[g, rows(mine), :] = own[:, g * GW:(g + 1) * GW]
    pl.semaphore_wait(barrier, 2)

    arrive = {}
    for g in range(ng):
        block = xg.at[g, rows(mine)]
        to_peer = remote(block, block, g_sem, peer, 0, g)
        launch(to_peer)
        to_mate = remote(block, block, g_sem, mate, 1, g)
        launch(to_mate)
        arrive[g] = (to_peer, to_mate)
    relays = []
    for g in range(ng):
        arrive[g][0].wait_recv()
        block = xg.at[g, rows(across)]
        relay = remote(block, block, g_sem, mate, 2, g)
        launch(relay)
        relays.append(relay)
    for g in range(ng):
        arrive[g][1].wait_recv()
        relays[g].wait_recv()
        xn[:, g * GW:(g + 1) * GW] = xg[g]

    for l in range(n_layers):
        last = l == n_layers - 1
        for j in range(n1):
            cols = pl.ds(j * BW1, BW1)
            loads1[l, j].wait()
            u = jnp.dot(xn[...], wv[2 * l, :, cols], preferred_element_type=jnp.float32)
            h[:, cols] = jax.nn.gelu(u, approximate=True).astype(jnp.bfloat16)

        d2d, ici, yq, ym, yr = {}, {}, {}, {}, {}
        for step in range(n2 + max(LAG_SUM[l], LAG_OUT[l], LAG_RELAY[l])):
            j = step
            if j < n2:
                cols = pl.ds(j * BW2, BW2)
                loads2[l, j].wait()
                part[l, j] = jnp.dot(h[...], wv[2 * l + 1, :, cols], preferred_element_type=jnp.float32)
                d2d[j] = remote(part.at[l, j, rows((1 - core) * 2, 2)], part_in.at[l, j],
                                d2d_sem, mate, l, j)
                launch(d2d[j])
            j = step - LAG_SUM[l]
            if 0 <= j < n2:
                d2d[j].wait_recv()
                sum_out[l, j] = part[l, j, rows(across), :] + part_in[l, j, rows(1 - chip), :]
                ici[j] = remote(sum_out.at[l, j], sum_in.at[l, j], ici_sem, peer, l, j)
                launch(ici[j])
            j = step - LAG_OUT[l]
            if 0 <= j < n2:
                cols = pl.ds(j * BW2, BW2)
                ici[j].wait_recv()
                total = part[l, j, rows(mine), :] + part_in[l, j, rows(chip), :] + sum_in[l, j]
                y = (x_own[:, cols].astype(jnp.float32) + total).astype(jnp.bfloat16)
                if last:
                    out_ref[:, cols] = y
                else:
                    x_own[:, cols] = y
                    yg[j, rows(mine), :] = y
                    block = yg.at[j, rows(mine)]
                    yq[j] = remote(block, block, y_sem, peer, 0, j)
                    launch(yq[j])
                    ym[j] = remote(block, block, y_sem, mate, 1, j)
                    launch(ym[j])
            j = step - LAG_RELAY[l]
            if not last and 0 <= j < n2:
                yq[j].wait_recv()
                block = yg.at[j, rows(across)]
                yr[j] = remote(block, block, y_sem, mate, 2, j)
                launch(yr[j])
        if not last:
            for j in range(n2):
                ym[j].wait_recv()
                yr[j].wait_recv()
            for b in range(4):
                r = slice(b * R, (b + 1) * R)
                full = jnp.concatenate([yg[j, r, :] for j in range(n2)], axis=1)
                xn[r, :] = normalize(full.astype(jnp.float32), gam[l + 1:l + 2, :])

    for copy in sends:
        copy.wait_send()


def solution(mesh):
    def local_stack(x_local, ln_gammas, w_in, w_out):
        R, width = x_local.shape
        n_layers, _, ff = w_in.shape
        S = 4 * R
        n1, n2, ng = ff // BW1, width // BW2, width // GW
        f32, bf16 = jnp.float32, jnp.bfloat16
        return pl.pallas_call(
            kernel,
            out_shape=jax.ShapeDtypeStruct((R, width), bf16),
            in_specs=[pl.BlockSpec(memory_space=pl.ANY)] * 4,
            out_specs=pl.BlockSpec(memory_space=pltpu.VMEM),
            scratch_shapes=[
                pltpu.VMEM((2 * n_layers, width, ff), bf16),
                pltpu.VMEM((R, width), bf16),
                pltpu.VMEM((n_layers, width), f32),
                pltpu.VMEM((ng, S, GW), bf16),
                pltpu.VMEM((S, width), bf16),
                pltpu.VMEM((S, ff), bf16),
                pltpu.VMEM((n_layers, n2, S, BW2), f32),
                pltpu.VMEM((n_layers, n2, 2 * R, BW2), f32),
                pltpu.VMEM((n_layers, n2, R, BW2), f32),
                pltpu.VMEM((n_layers, n2, R, BW2), f32),
                pltpu.VMEM((n2, S, BW2), bf16),
                pltpu.SemaphoreType.DMA((2,)),
                pltpu.SemaphoreType.DMA((n_layers, n1)),
                pltpu.SemaphoreType.DMA((n_layers, n2)),
                pltpu.SemaphoreType.DMA((2, 3, ng)),
                pltpu.SemaphoreType.DMA((2, n_layers, n2)),
                pltpu.SemaphoreType.DMA((2, n_layers, n2)),
                pltpu.SemaphoreType.DMA((2, 3, n2)),
            ],
            compiler_params=pltpu.CompilerParams(
                collective_id=0, has_side_effects=True, vmem_limit_bytes=66_000_000),
            name="mlp_stack",
        )(x_local, ln_gammas, w_in, w_out)

    return jax.shard_map(
        local_stack,
        mesh=mesh,
        in_specs=(P(('data', 'tp'), None), P(None, None), P(None, None, 'tp'), P(None, 'tp', None)),
        out_specs=P(('data', 'tp'), None),
        check_vma=False,
    )
```

```python
import functools
import jax
import jax.numpy as jnp
from jax import lax
from jax.experimental import pallas as pl
from jax.experimental.pallas import tpu as pltpu
from jax.sharding import PartitionSpec as P

LN_EPS = 1e-6
MESH = pl.DeviceIdType.MESH

BW1 = 512
BW2 = 512
GW = 1280
MXU_ROWS = 128
LAG_SUM = (1, 2)
LAG_OUT = (3, 5)
LAG_RELAY = (5, 5)


def normalize(rows_f32, gamma_row):
    mean_val = jnp.mean(rows_f32, axis=-1, keepdims=True)
    centered = rows_f32 - mean_val
    var_val = jnp.mean(centered * centered, axis=-1, keepdims=True)
    return (centered * lax.rsqrt(var_val + LN_EPS) * gamma_row).astype(jnp.bfloat16)


def kernel(x_hbm, gam_hbm, w_in, w_out, out_ref,
           wv, x_own, gam, xg, xn, h, part, part_in, sum_out, sum_in, yg,
           lsem, wsem1, wsem2, g_sem, d2d_sem, ici_sem, y_sem):
    n_layers, width, ff = w_in.shape
    n1, n2, ng = ff // BW1, width // BW2, width // GW
    me = lax.axis_index("tp")
    chip, core = lax.div(me, 2), lax.rem(me, 2)
    mate = {"tp": chip * 2 + (1 - core)}
    peer = {"tp": (1 - chip) * 2 + core}
    R = x_own.shape[0]
    S = 4 * R
    xn[S:, :] = jnp.zeros_like(xn[S:, :])
    h[S:, :] = jnp.zeros_like(h[S:, :])
    mine = core * 2 + chip
    across = core * 2 + (1 - chip)

    def rows(block, n=1):
        return pl.ds(pl.multiple_of(block * R, R), n * R)

    load_x = pltpu.make_async_copy(x_hbm, x_own, lsem.at[0])
    load_g = pltpu.make_async_copy(gam_hbm, gam, lsem.at[1])
    load_x.start()
    load_g.start()
    loads1, loads2 = {}, {}
    for l in range(n_layers):
        for j in range(n1):
            cols = pl.ds(j * BW1, BW1)
            loads1[l, j] = pltpu.make_async_copy(
                w_in.at[l, :, cols], wv.at[2 * l, :, cols], wsem1.at[l, j])
            loads1[l, j].start(priority=1)
        for j in range(n2):
            cols = pl.ds(j * BW2, BW2)
            loads2[l, j] = pltpu.make_async_copy(
                w_out.at[l, :, cols], wv.at[2 * l + 1, :, cols], wsem2.at[l, j])
            loads2[l, j].start(priority=1)

    barrier = pltpu.get_barrier_semaphore()
    for other in (mate, peer):
        pl.semaphore_signal(barrier, inc=1, device_id=other, device_id_type=MESH)

    sends = []

    def remote(src, dst, sems, device, *idx):
        copy = pltpu.make_async_remote_copy(
            src_ref=src, dst_ref=dst, send_sem=sems.at[(0,) + idx], recv_sem=sems.at[(1,) + idx],
            device_id=device, device_id_type=MESH)
        return copy

    def launch(copy):
        copy.start()
        sends.append(copy)

    with jax.named_scope('wait_x'):
        load_x.wait()
        load_g.wait()
    own = normalize(x_own[...].astype(jnp.float32), gam[0:1, :])
    for g in range(ng):
        xg[g, rows(mine), :] = own[:, g * GW:(g + 1) * GW]
    with jax.named_scope('barrier'):
        pl.semaphore_wait(barrier, 2)

    arrive = {}
    for g in range(ng):
        block = xg.at[g, rows(mine)]
        to_peer = remote(block, block, g_sem, peer, 0, g)
        launch(to_peer)
        to_mate = remote(block, block, g_sem, mate, 1, g)
        launch(to_mate)
        arrive[g] = (to_peer, to_mate)
    relays = []
    for g in range(ng):
        with jax.named_scope(f'ag0_peer{g}'):
            arrive[g][0].wait_recv()
        block = xg.at[g, rows(across)]
        relay = remote(block, block, g_sem, mate, 2, g)
        launch(relay)
        relays.append(relay)
    for g in range(ng):
        with jax.named_scope(f'ag0_mate{g}'):
            arrive[g][1].wait_recv()
        with jax.named_scope(f'ag0_relay{g}'):
            relays[g].wait_recv()
        xn[0:S, g * GW:(g + 1) * GW] = xg[g]

    for l in range(n_layers):
        last = l == n_layers - 1
        for j in range(n1):
            cols = pl.ds(j * BW1, BW1)
            with jax.named_scope(f'w1_{l}_{j}'):
                loads1[l, j].wait()
            u = jnp.dot(xn[...], wv[2 * l, :, cols], preferred_element_type=jnp.float32)[:S]
            h[0:S, cols] = jax.nn.gelu(u, approximate=True).astype(jnp.bfloat16)

        d2d, ici, yq, ym, yr = {}, {}, {}, {}, {}
        for step in range(n2 + max(LAG_SUM[l], LAG_OUT[l], LAG_RELAY[l])):
            j = step
            if j < n2:
                cols = pl.ds(j * BW2, BW2)
                with jax.named_scope(f'w2_{l}_{j}'):
                    loads2[l, j].wait()
                part[l, j] = jnp.dot(h[...], wv[2 * l + 1, :, cols], preferred_element_type=jnp.float32)[:S]
                d2d[j] = remote(part.at[l, j, rows((1 - core) * 2, 2)], part_in.at[l, j],
                                d2d_sem, mate, l, j)
                launch(d2d[j])
            j = step - LAG_SUM[l]
            if 0 <= j < n2:
                with jax.named_scope(f'd2d_{l}_{j}'):
                    d2d[j].wait_recv()
                sum_out[l, j] = part[l, j, rows(across), :] + part_in[l, j, rows(1 - chip), :]
                ici[j] = remote(sum_out.at[l, j], sum_in.at[l, j], ici_sem, peer, l, j)
                launch(ici[j])
            j = step - LAG_OUT[l]
            if 0 <= j < n2:
                cols = pl.ds(j * BW2, BW2)
                with jax.named_scope(f'ici_{l}_{j}'):
                    ici[j].wait_recv()
                total = part[l, j, rows(mine), :] + part_in[l, j, rows(chip), :] + sum_in[l, j]
                y = (x_own[:, cols].astype(jnp.float32) + total).astype(jnp.bfloat16)
                if last:
                    out_ref[:, cols] = y
                else:
                    x_own[:, cols] = y
                    yg[j, rows(mine), :] = y
                    block = yg.at[j, rows(mine)]
                    yq[j] = remote(block, block, y_sem, peer, 0, j)
                    launch(yq[j])
                    ym[j] = remote(block, block, y_sem, mate, 1, j)
                    launch(ym[j])
            j = step - LAG_RELAY[l]
            if not last and 0 <= j < n2:
                with jax.named_scope(f'yq_{l}_{j}'):
                    yq[j].wait_recv()
                block = yg.at[j, rows(across)]
                yr[j] = remote(block, block, y_sem, mate, 2, j)
                launch(yr[j])
        if not last:
            for j in range(n2):
                with jax.named_scope(f'ym_{l}_{j}'):
                    ym[j].wait_recv()
                with jax.named_scope(f'yr_{l}_{j}'):
                    yr[j].wait_recv()
            for b in range(4):
                r = slice(b * R, (b + 1) * R)
                full = jnp.concatenate([yg[j, r, :] for j in range(n2)], axis=1)
                xn[r, :] = normalize(full.astype(jnp.float32), gam[l + 1:l + 2, :])

    with jax.named_scope('drain'):
        for copy in sends:
            copy.wait_send()


def solution(mesh):
    def local_stack(x_local, ln_gammas, w_in, w_out):
        R, width = x_local.shape
        n_layers, _, ff = w_in.shape
        S = 4 * R
        n1, n2, ng = ff // BW1, width // BW2, width // GW
        f32, bf16 = jnp.float32, jnp.bfloat16
        return pl.pallas_call(
            kernel,
            out_shape=jax.ShapeDtypeStruct((R, width), bf16),
            in_specs=[pl.BlockSpec(memory_space=pl.ANY)] * 4,
            out_specs=pl.BlockSpec(memory_space=pltpu.VMEM),
            scratch_shapes=[
                pltpu.VMEM((2 * n_layers, width, ff), bf16),
                pltpu.VMEM((R, width), bf16),
                pltpu.VMEM((n_layers, width), f32),
                pltpu.VMEM((ng, S, GW), bf16),
                pltpu.VMEM((MXU_ROWS, width), bf16),
                pltpu.VMEM((MXU_ROWS, ff), bf16),
                pltpu.VMEM((n_layers, n2, S, BW2), f32),
                pltpu.VMEM((n_layers, n2, 2 * R, BW2), f32),
                pltpu.VMEM((n_layers, n2, R, BW2), f32),
                pltpu.VMEM((n_layers, n2, R, BW2), f32),
                pltpu.VMEM((n2, S, BW2), bf16),
                pltpu.SemaphoreType.DMA((2,)),
                pltpu.SemaphoreType.DMA((n_layers, n1)),
                pltpu.SemaphoreType.DMA((n_layers, n2)),
                pltpu.SemaphoreType.DMA((2, 3, ng)),
                pltpu.SemaphoreType.DMA((2, n_layers, n2)),
                pltpu.SemaphoreType.DMA((2, n_layers, n2)),
                pltpu.SemaphoreType.DMA((2, 3, n2)),
            ],
            compiler_params=pltpu.CompilerParams(
                collective_id=0, has_side_effects=True, vmem_limit_bytes=66_000_000),
            name="mlp_stack",
        )(x_local, ln_gammas, w_in, w_out)

    return jax.shard_map(
        local_stack,
        mesh=mesh,
        in_specs=(P(('data', 'tp'), None), P(None, None), P(None, None, 'tp'), P(None, 'tp', None)),
        out_specs=P(('data', 'tp'), None),
        check_vma=False,
    )
```
